32 devices in a mesh: row: 8 (over z, x), col: 4 (over y, core).
Axes of the slice: x: 2, y: 2, z: 4, core: 2. Of those that a mesh axis runs over, the one named last changes fastest.
Arguments:
- normal_matrix: float32 [9216, 9216], P('row', 'col'), may hold values from -1 to 6, as said below
- right_side: float32 [9216, 64], P('col'), may hold values from -6 to 6
- tile_inverse: float32 [72, 128, 128], P('col'), may hold values from -1 to 3.5, as said below
- order_ids: int32 [9216], P('col'), may hold values from 0 to 96, never falling along the last dimension, each value on 1 to 194 neighbouring positions
Outputs:
- solution: float32 [9216, 64], P('col')
- residual: float32 [9216, 64], P('col')
The draws below stay inside these ranges and needn't reach their ends.
Inputs may be any that keep to these rules, and one draw needn't show every extreme that they name: `normal_matrix`: symmetric and positive definite. `tile_inverse`: each tile symmetric, every principal submatrix of it positive definite. `order_ids`: never falling along the coefficients; each order holds 1 to 194 coefficients.
All inputs are finite; a program needn't handle non-finite values.
Results may differ from the reference program's by a relative error of at most 0.0003.
Values sent between devices are 32-bit elements; how exact they have to be, the bound alone decides.
A program may use at most 64 MiB of HBM per device.

```python
import math
import jax
import jax.numpy as jnp
import numpy as np
from jax import lax

NUM = 9216
ORDERS = 97
ORDER_MOST = 194
BLK = 128
NRHS = 64
ITERS = 2


def draw_normal_matrix(key, part):
    first, second = jax.random.split(jax.random.fold_in(key, 11))
    raw = jax.random.normal(first, (NUM, NUM), jnp.float32)
    symmetric = (raw + raw.T) * (0.5 / math.sqrt(NUM))
    diagonal = jax.random.uniform(second, (NUM,), jnp.float32, 2.0, 4.0)
    return symmetric + jnp.diag(diagonal)


def draw_tile_inverse(key, part):
    first, second = jax.random.split(jax.random.fold_in(key, 23))
    raw = jax.random.normal(first, (NUM // BLK, BLK, BLK), jnp.float32)
    symmetric = (raw + jnp.swapaxes(raw, 1, 2)) * (0.3 / math.sqrt(BLK))
    diagonal = jax.random.uniform(second, (NUM // BLK, BLK), jnp.float32, 1.0, 3.0)
    eye = jnp.eye(BLK, dtype=jnp.float32)
    return symmetric + diagonal[:, :, None] * eye[None, :, :]


def block_levels(rng, dims, cuts, least, top_value):
    loudness = 1.0
    for dim, blocks in cuts:
        steps = jax.random.uniform(jax.random.fold_in(jax.random.fold_in(rng, 6), dim), (blocks,), jnp.float32, least / len(cuts), top_value / len(cuts))
        loudness = loudness * jnp.repeat(jnp.exp(steps), dims[dim] // blocks).reshape((-1,) + (1,) * (len(dims) - 1 - dim))
    return loudness


def profile(count, total, limit, lean):
    loads = [(1 << 20) // math.isqrt(standing ** lean) + 1 for standing in range(2, count + 1)]
    surplus, given = total - limit - (count - 1), [1] * (count - 1)
    while surplus > 0:
        free = [i for i in range(count - 1) if given[i] < limit]
        mass, remaining = sum([loads[i] for i in free]), surplus
        for i in free:
            extra = min(limit - given[i], max(1, remaining * loads[i] // mass), surplus)
            given[i] = given[i] + extra
            surplus = surplus - extra
    return np.array([limit] + given)


def ragged(own_key, number_of, total, bound, lean):
    if number_of == 2:
        one = jax.random.randint(own_key, (), max(1, total - bound), min(bound, total - 1) + 1)
        return jnp.stack([one, total - one])
    sizes = jnp.asarray(profile(number_of, total, bound, lean), jnp.int32)
    pairs = (number_of - 1) // 2
    giver, sink = sizes[1:1 + 2 * pairs:2], sizes[2:2 + 2 * pairs:2]
    margin = jnp.minimum(giver - 1, bound - sink)
    passed = jax.random.randint(jax.random.fold_in(own_key, 1), (pairs,), 0, 1 << 20) % (margin + 1)
    sizes = sizes.at[1:1 + 2 * pairs:2].set(giver - passed).at[2:2 + 2 * pairs:2].set(sink + passed)
    return sizes[jax.random.permutation(jax.random.fold_in(own_key, 2), number_of)]


def centred(stream_key, shape, deviation, reach, shards=(), kind=jnp.bfloat16):
    values = deviation * jax.random.normal(stream_key, shape, jnp.float32)
    if shards:
        values = values * block_levels(stream_key, shape, shards, -0.22, 0.18)
    return jnp.clip(values, -reach, reach).astype(kind)


def setup_inputs(seed: int = 0) -> dict:
    keys = jax.random.split(jax.random.key(seed), 5)
    normal_matrix = draw_normal_matrix(jax.random.fold_in(keys[4], 71), 0)
    right_side = centred(keys[1], (NUM, NRHS), 1.0, 6.0, ((0, 4),), jnp.float32)
    tile_inverse = draw_tile_inverse(jax.random.fold_in(keys[4], 71), 0)
    order_ids = jnp.searchsorted(jnp.cumsum(ragged(keys[3], ORDERS, NUM, ORDER_MOST, 0)), jnp.arange(NUM), side="right").astype(jnp.int32)
    return {"normal_matrix": normal_matrix, "right_side": right_side, "tile_inverse": tile_inverse, "order_ids": order_ids}


def apply_precond(tile_inverse, order_ids, vector):
    count = tile_inverse.shape[0]
    width = tile_inverse.shape[1]
    order_tile = order_ids.reshape(count, width)
    same_order = order_tile[:, :, None] == order_tile[:, None, :]
    masked = jnp.where(same_order, tile_inverse, jnp.float32(0.0))
    pieces = vector.reshape(count, width, vector.shape[1])
    result = jnp.einsum("tij,tjk->tik", masked, pieces, precision=lax.Precision.HIGHEST)
    return result.reshape(vector.shape)


def reference(normal_matrix, right_side, tile_inverse, order_ids):
    def apply_matrix(vector):
        return jnp.dot(normal_matrix, vector, precision=lax.Precision.HIGHEST, preferred_element_type=jnp.float32)

    solution = jnp.zeros_like(right_side)
    residual = right_side
    precond_res = apply_precond(tile_inverse, order_ids, residual)
    image_res = apply_matrix(precond_res)
    image_dir = jnp.zeros_like(right_side)
    precond_dir = jnp.zeros_like(right_side)
    residual_dir = jnp.zeros_like(right_side)
    direction = jnp.zeros_like(right_side)
    gamma_prev = jnp.ones((right_side.shape[1],), jnp.float32)
    alpha_prev = jnp.ones((right_side.shape[1],), jnp.float32)
    for iteration in range(ITERS):
        gamma_now = jnp.sum(residual * precond_res, axis=0)
        delta_now = jnp.sum(image_res * precond_res, axis=0)
        precond_img = apply_precond(tile_inverse, order_ids, image_res)
        image_img = apply_matrix(precond_img)
        if iteration == 0:
            beta_ratio = jnp.zeros_like(gamma_now)
            step_size = gamma_now / delta_now
        else:
            beta_ratio = gamma_now / gamma_prev
            step_size = gamma_now / (delta_now - beta_ratio * gamma_now / alpha_prev)
        image_dir = image_img + beta_ratio * image_dir
        precond_dir = precond_img + beta_ratio * precond_dir
        residual_dir = image_res + beta_ratio * residual_dir
        direction = precond_res + beta_ratio * direction
        solution = solution + step_size * direction
        residual = residual - step_size * residual_dir
        precond_res = precond_res - step_size * precond_dir
        image_res = image_res - step_size * image_dir
        gamma_prev = gamma_now
        alpha_prev = step_size
    return solution, residual
```

```python
import functools

import jax
import jax.numpy as jnp
from jax import lax
from jax.experimental import pallas as pl
from jax.experimental.pallas import tpu as pltpu
from jax.sharding import PartitionSpec as P

ITERS = 2
MESH = pl.DeviceIdType.MESH
NEAR_LAG = 3
OWN_LAG = 5
SIDE_LAG = 8


def masked_tiles(tile_inverse, order_ids):
    count = tile_inverse.shape[0]
    width = tile_inverse.shape[1]
    order_tile = order_ids.reshape(count, width)
    same_order = order_tile[:, :, None] == order_tile[:, None, :]
    return jnp.where(same_order, tile_inverse, jnp.float32(0.0))


def apply_precond(tile_inverse, order_ids, vector):
    count = tile_inverse.shape[0]
    width = tile_inverse.shape[1]
    masked = masked_tiles(tile_inverse, order_ids)
    pieces = vector.reshape(count, width, vector.shape[1])
    result = jnp.einsum("tij,tjk->tik", masked, pieces, precision=lax.Precision.HIGHEST)
    return result.reshape(vector.shape)


def plain_body(normal_matrix, right_side, tile_inverse, order_ids):
    block_rows = normal_matrix.shape[0]

    def apply_matrix(vector):
        first_row = lax.axis_index("row") * block_rows
        gathered = lax.all_gather(vector, "col", axis=0, tiled=True)
        row_piece = lax.dynamic_slice_in_dim(gathered, first_row, block_rows, 0)
        partial_value = lax.dot_general(
            normal_matrix,
            row_piece,
            (((0,), (0,)), ((), ())),
            precision=lax.Precision.HIGHEST,
            preferred_element_type=jnp.float32,
        )
        return lax.psum(partial_value, "row")

    solution = jnp.zeros_like(right_side)
    residual = right_side
    precond_res = apply_precond(tile_inverse, order_ids, residual)
    image_res = apply_matrix(precond_res)
    image_dir = jnp.zeros_like(right_side)
    precond_dir = jnp.zeros_like(right_side)
    residual_dir = jnp.zeros_like(right_side)
    direction = jnp.zeros_like(right_side)
    gamma_prev = jnp.ones((right_side.shape[1],), jnp.float32)
    alpha_prev = jnp.ones((right_side.shape[1],), jnp.float32)
    for iteration in range(ITERS):
        gamma_now, delta_now = lax.psum(
            (jnp.sum(residual * precond_res, axis=0), jnp.sum(image_res * precond_res, axis=0)),
            "col",
        )
        precond_img = apply_precond(tile_inverse, order_ids, image_res)
        image_img = apply_matrix(precond_img)
        if iteration == 0:
            beta_ratio = jnp.zeros_like(gamma_now)
            step_size = gamma_now / delta_now
        else:
            beta_ratio = gamma_now / gamma_prev
            step_size = gamma_now / (delta_now - beta_ratio * gamma_now / alpha_prev)
        image_dir = image_img + beta_ratio * image_dir
        precond_dir = precond_img + beta_ratio * precond_dir
        residual_dir = image_res + beta_ratio * residual_dir
        direction = precond_res + beta_ratio * direction
        solution = solution + step_size * direction
        residual = residual - step_size * residual_dir
        precond_res = precond_res - step_size * precond_dir
        image_res = image_res - step_size * image_dir
        gamma_prev = gamma_now
        alpha_prev = step_size
    return (solution, residual)


def halves(value):
    high = value.astype(jnp.bfloat16)
    low = (value - high.astype(jnp.float32)).astype(jnp.bfloat16)
    return high, low


def split(value):
    return jnp.concatenate(halves(value), axis=0)


def times(left, right):
    return lax.dot_general(
        left, right, (((1,), (0,)), ((), ())), preferred_element_type=jnp.float32
    )


def times_transposed(left, right):
    return lax.dot_general(
        left, right, (((1,), (1,)), ((), ())), preferred_element_type=jnp.float32
    )


def fold(product, rows, columns):
    both = product[:rows] + product[rows:]
    return both[:, :columns] + both[:, columns:]


def kernel(
    depth, width,
    a_ref, tile_ref, b_ref, ids_ref,
    u_out, m_out, w_out, n_out, s_out,
    a_buf, a_split, tile_buf, tile_split, v_split, m_split, b_buf, u_buf, m_buf,
    part, near, half, far, done, image, acc,
    sums, dot_own, dot_in, delta_own, delta_in, ids_buf,
    a_sem, in_sem, out_sem, near_sem, far_sem, line_sem, side_sem,
    near_send, far_send, fan_send, relay_send, dot_send, dot_recv, delta_send, delta_recv,
):
    my_row, my_col = lax.axis_index("row"), lax.axis_index("col")
    place, lane = my_row // 2, lax.rem(my_row, 2)
    core = lax.rem(my_col, 2)
    partner = my_col + 1 - 2 * core
    across = lax.rem(my_col + 2, 4)
    side = my_row + 1 - 2 * lane
    owner = place == my_col
    owner_chip = place // 2 == my_col // 2
    helper = jnp.logical_and(owner_chip, jnp.logical_not(owner))
    others = jnp.logical_not(owner)
    above, below = place < depth - 1, place > 0
    nrhs, block_cols = b_buf.shape
    block_rows = acc.shape[1]
    hh = nrhs // 2
    tiles = block_cols // width
    steps = block_rows // width
    mine = pl.ds(pl.multiple_of(core * hh, hh), hh)
    other = pl.ds(pl.multiple_of((1 - core) * hh, hh), hh)

    def fetch(i):
        return pltpu.make_async_copy(a_ref.at[pl.ds(i * width, width)], a_buf.at[i], a_sem.at[i])

    fetch_b = pltpu.make_async_copy(b_ref, b_buf, in_sem.at[0])
    fetch_tiles = pltpu.make_async_copy(tile_ref, tile_buf, in_sem.at[1])
    fetch_tiles.start()
    fetch_b.start()
    for i in range(steps):
        fetch(i).start()

    barrier = pltpu.get_barrier_semaphore()

    def greet(row, col):
        pl.semaphore_signal(barrier, inc=1, device_id=(row, col), device_id_type=MESH)

    for shift in range(1, 4):
        greet(my_row, lax.rem(my_col + shift, 4))
    greet(side, my_col)
    greet(2 * my_col + 1 - lane, my_col)

    @pl.when(others)
    def _():
        greet(2 * my_col + lane, my_col)

    @pl.when(place > my_col)
    def _():
        greet(my_row - 2, my_col)

    @pl.when(place < my_col)
    def _():
        greet(my_row + 2, my_col)

    @pl.when(jnp.logical_or(place == my_col + 1, place == my_col - 1))
    def _():
        greet(2 * my_col + lane, partner)

    @pl.when(owner)
    def _():
        greet(side, partner)

    goes_up = jnp.logical_and(place >= my_col, above)
    goes_down = jnp.logical_and(place <= my_col, below)

    def one(flag):
        return jnp.where(flag, 1, 0)

    def meet():
        awaited = 4 + one(goes_up) + one(goes_down)
        awaited += jnp.where(helper, 1 + one(above) + one(below), 0)
        awaited += jnp.where(owner, 2 * depth - 1, 0)
        pl.semaphore_wait(barrier, awaited)

    def lanes_at(t):
        return pl.ds(pl.multiple_of(t * width, width), width)

    def cut(q):
        return pl.ds(q * width, width)

    def lanes_of(block, q):
        return lanes_at(block * steps + q)

    def near_chunk(turn, q):
        return pltpu.make_async_remote_copy(
            src_ref=part.at[turn, other, cut(q)], dst_ref=near.at[turn, :, cut(q)],
            send_sem=near_send.at[turn], recv_sem=near_sem.at[turn, q],
            device_id=(my_row, partner), device_id_type=MESH,
        )

    def far_chunk(turn, q):
        return pltpu.make_async_remote_copy(
            src_ref=half.at[turn, :, cut(q)], dst_ref=far.at[turn, :, cut(q)],
            send_sem=far_send.at[turn], recv_sem=far_sem.at[turn, q],
            device_id=(my_row, across), device_id_type=MESH,
        )

    def fan_chunk(turn, q, way, row, sem):
        return pltpu.make_async_remote_copy(
            src_ref=done.at[turn, :, cut(q)], dst_ref=image.at[turn, mine, lanes_of(lane, q)],
            send_sem=fan_send.at[turn, way], recv_sem=sem.at[turn, q],
            device_id=(row, place), device_id_type=MESH,
        )

    def relay_chunk(turn, q, way, row, sem):
        return pltpu.make_async_remote_copy(
            src_ref=image.at[turn, :, lanes_of(lane, q)], dst_ref=image.at[turn, :, lanes_of(lane, q)],
            send_sem=relay_send.at[turn, way], recv_sem=sem.at[turn, q],
            device_id=(row, my_col), device_id_type=MESH,
        )

    def stage1(turn, q):
        near_chunk(turn, q).wait_recv()
        half[turn, :, cut(q)] = part[turn, mine, cut(q)] + near[turn, :, cut(q)]

        @pl.when(jnp.logical_not(owner_chip))
        def _():
            far_chunk(turn, q).start()

    def stage2(turn, q):
        @pl.when(owner_chip)
        def _():
            far_chunk(turn, q).wait_recv()
            total = half[turn, :, cut(q)] + far[turn, :, cut(q)]
            done[turn, :, cut(q)] = total

            @pl.when(above)
            def _():
                fan_chunk(turn, q, 0, my_row + 2, line_sem).start()

            @pl.when(below)
            def _():
                fan_chunk(turn, q, 1, my_row - 2, line_sem).start()

            fan_chunk(turn, q, 2, side, side_sem).start()

            @pl.when(helper)
            def _():
                fan_chunk(turn, q, 3, my_row, line_sem).start()

            @pl.when(owner)
            def _():
                image[turn, mine, lanes_of(lane, q)] = total

    def own(turn, q):
        @pl.when(owner)
        def _():
            pltpu.make_async_remote_copy(
                src_ref=done.at[turn, :, cut(q)], dst_ref=image.at[turn, other, lanes_of(lane, q)],
                send_sem=fan_send.at[turn, 3], recv_sem=line_sem.at[turn, q],
                device_id=(my_row, partner), device_id_type=MESH,
            ).wait_recv()

        @pl.when(others)
        def _():
            relay_chunk(turn, q, 0, my_row, line_sem).wait_recv()

            @pl.when(goes_up)
            def _():
                relay_chunk(turn, q, 0, my_row + 2, line_sem).start()

            @pl.when(goes_down)
            def _():
                relay_chunk(turn, q, 0, my_row - 2, line_sem).start()

            relay_chunk(turn, q, 1, side, side_sem).start()

    def beside(turn, q):
        pltpu.make_async_remote_copy(
            src_ref=image.at[turn, :, lanes_of(1 - lane, q)], dst_ref=image.at[turn, :, lanes_of(1 - lane, q)],
            send_sem=relay_send.at[turn, 1], recv_sem=side_sem.at[turn, q],
            device_id=(side, my_col), device_id_type=MESH,
        ).wait_recv()

    def finish(turn):
        near_all = pltpu.make_async_remote_copy(
            src_ref=part.at[turn, other], dst_ref=near.at[turn],
            send_sem=near_send.at[turn], recv_sem=near_sem.at[turn, 0],
            device_id=(my_row, partner), device_id_type=MESH,
        )
        near_all.wait_send()

        def fan_all(way):
            return pltpu.make_async_remote_copy(
                src_ref=done.at[turn], dst_ref=far.at[turn],
                send_sem=fan_send.at[turn, way], recv_sem=line_sem.at[turn, 0],
                device_id=(side, my_col), device_id_type=MESH,
            )

        def relay_all(way):
            return pltpu.make_async_remote_copy(
                src_ref=part.at[turn], dst_ref=part.at[turn],
                send_sem=relay_send.at[turn, way], recv_sem=line_sem.at[turn, 0],
                device_id=(side, my_col), device_id_type=MESH,
            )

        @pl.when(jnp.logical_not(owner_chip))
        def _():
            pltpu.make_async_remote_copy(
                src_ref=half.at[turn], dst_ref=far.at[turn],
                send_sem=far_send.at[turn], recv_sem=far_sem.at[turn, 0],
                device_id=(my_row, across), device_id_type=MESH,
            ).wait_send()

        @pl.when(owner_chip)
        def _():
            @pl.when(above)
            def _():
                fan_all(0).wait_send()

            @pl.when(below)
            def _():
                fan_all(1).wait_send()

            fan_all(2).wait_send()

            @pl.when(helper)
            def _():
                fan_all(3).wait_send()

        @pl.when(others)
        def _():
            @pl.when(jnp.logical_or(goes_up, goes_down))
            def _():
                relay_all(0).wait_send()

            relay_all(1).wait_send()

    def dot_row():
        return jnp.sum(sums[...].T, axis=0, keepdims=True)

    def exchange(turn, row):
        dot_own[turn] = jnp.broadcast_to(row, dot_own.shape[1:])
        for shift in (2, 1, 3):
            pltpu.make_async_remote_copy(
                src_ref=dot_own.at[turn], dst_ref=dot_in.at[turn, shift - 1],
                send_sem=dot_send.at[turn], recv_sem=dot_recv.at[turn],
                device_id=(my_row, lax.rem(my_col + shift, 4)), device_id_type=MESH,
            ).start()

    def exchanged(turn):
        pltpu.make_async_remote_copy(
            src_ref=dot_in.at[turn], dst_ref=dot_in.at[turn],
            send_sem=dot_send.at[turn], recv_sem=dot_recv.at[turn],
            device_id=(my_row, partner), device_id_type=MESH,
        ).wait()
        total = (dot_own[turn] + dot_in[turn, 1]) + (dot_in[turn, 0] + dot_in[turn, 2])
        across_lanes = jnp.broadcast_to(total[0:1], (2 * nrhs, width)).T
        return across_lanes[:nrhs], across_lanes[nrhs:]

    ids_buf[...] = jnp.zeros_like(ids_buf)
    ids_buf[0:tiles] = ids_ref[...].astype(jnp.float32)
    ids_across = ids_buf[...].T
    fetch_tiles.wait()
    for t in range(tiles):
        same = ids_across[:, t : t + 1] == ids_buf[t : t + 1]
        tile_split[t] = jnp.concatenate(halves(jnp.where(same, tile_buf[t], 0.0)), axis=1)
    fetch_b.wait()
    gamma = jnp.zeros((nrhs, width), jnp.float32)
    for t in range(tiles):
        value = b_buf[:, cut(t)]
        product = fold(times(split(value), tile_split[t]), nrhs, width)
        u_buf[:, cut(t)] = product
        v_split[:, cut(t)] = split(product)
        gamma += value * product
    sums[:nrhs] = gamma
    sums[nrhs:] = jnp.zeros_like(gamma)

    for q in range(steps):
        fetch(q).wait()
        a_split[q] = split(a_buf[q])
        part[0, :, cut(q)] = fold(times_transposed(v_split[...], a_split[q]), nrhs, width)
        if q == 0:
            meet()
        near_chunk(0, q).start()
        if q >= NEAR_LAG:
            stage1(0, q - NEAR_LAG)
    for q in range(steps - NEAR_LAG, steps):
        stage1(0, q)
    write_u = pltpu.make_async_copy(u_buf, u_out, out_sem.at[0])
    write_u.start()

    acc[...] = jnp.zeros_like(acc)

    def take(block, q, slot):
        lanes = lanes_of(block, q)
        value = image[0, :, lanes]
        product = fold(times(split(value), tile_split[block * steps + q]), nrhs, width)
        m_buf[:, lanes] = product
        m_split[slot] = split(product)
        sums[nrhs:] += value * u_buf[:, lanes]
        return slot, lanes

    def update(taken, i):
        product = None
        for slot, lanes in taken:
            term = times_transposed(m_split[slot], a_split[i, :, lanes])
            product = term if product is None else product + term
        return acc[:, cut(i)] + fold(product, nrhs, width)

    taken = []
    for tick in range(steps + SIDE_LAG):
        if tick < steps:
            stage2(0, tick)
        q, r = tick - OWN_LAG, tick - SIDE_LAG
        if 0 <= q < steps:
            own(0, q)
        if 0 <= r < steps:
            beside(0, r)
        if taken:
            for i in range(steps):
                acc[:, cut(i)] = update(taken, i)
        slot = 2 * (tick % 2)
        taken = []
        if 0 <= q < steps:
            taken.append(take(lane, q, slot))
        if 0 <= r < steps:
            taken.append(take(1 - lane, r, slot + 1))
    for i in range(steps):
        part[1, :, cut(i)] = update(taken, i)
        near_chunk(1, i).start()
    exchange(0, dot_row())
    write_m = pltpu.make_async_copy(m_buf, m_out, out_sem.at[1])
    write_m.start()
    write_w = pltpu.make_async_copy(image.at[0], w_out, out_sem.at[2])
    write_w.start()
    for q in range(steps):
        stage1(1, q)
    gamma0, delta0 = exchanged(0)
    alpha0 = gamma0 / delta0
    gamma = jnp.zeros((nrhs, width), jnp.float32)
    for t in range(tiles):
        lanes = cut(t)
        res = b_buf[:, lanes] - alpha0 * image[0, :, lanes]
        pre = u_buf[:, lanes] - alpha0 * m_buf[:, lanes]
        gamma += res * pre
    sums[:nrhs] = gamma
    sums[nrhs:] = jnp.zeros_like(gamma)

    def write_n(block, q):
        lanes = lanes_of(block, q)
        return pltpu.make_async_copy(image.at[1, :, lanes], n_out.at[:, lanes], out_sem.at[3])

    def deltas():
        row = dot_row()
        upper = lax.broadcasted_iota(jnp.int32, (1, width), 1) >= nrhs

        @pl.when(owner)
        def _():
            message = jnp.broadcast_to(jnp.where(upper, row, 0.0), delta_in.shape[1:])
            delta_in[lane] = message
            for i in range(2 * depth - 1):
                delta_own[i] = message
                pltpu.make_async_remote_copy(
                    src_ref=delta_own.at[i], dst_ref=delta_in.at[lane],
                    send_sem=delta_send.at[0], recv_sem=delta_recv.at[0],
                    device_id=(lax.rem(my_row + i + 1, 2 * depth), my_col), device_id_type=MESH,
                ).start()

        return row, upper

    for tick in range(steps + SIDE_LAG):
        if tick < steps:
            stage2(1, tick)
        q, r = tick - OWN_LAG, tick - SIDE_LAG
        if 0 <= q < steps:
            own(1, q)
            write_n(lane, q).start()

            @pl.when(owner)
            def _():
                lanes = lanes_of(lane, q)
                img = image[0, :, lanes] - alpha0 * image[1, :, lanes]
                sums[nrhs:] += img * (u_buf[:, lanes] - alpha0 * m_buf[:, lanes])

        if q == steps - 1:
            row, upper = deltas()
        if 0 <= r < steps:
            beside(1, r)
            write_n(1 - lane, r).start()

    def delta_copy(slots):
        return pltpu.make_async_remote_copy(
            src_ref=slots, dst_ref=slots, send_sem=delta_send.at[0], recv_sem=delta_recv.at[0],
            device_id=(side, my_col), device_id_type=MESH,
        )

    @pl.when(owner)
    def _():
        delta_copy(delta_in.at[1 - lane]).wait_recv()

    @pl.when(others)
    def _():
        delta_copy(delta_in).wait_recv()

    exchange(1, jnp.where(upper, (delta_in[0] + delta_in[1])[0:1], row))
    finish(0)
    finish(1)
    write_u.wait()
    write_m.wait()
    write_w.wait()
    pltpu.make_async_copy(image.at[1], n_out, out_sem.at[3]).wait()

    @pl.when(owner)
    def _():
        delta_copy(delta_own).wait_send()

    gamma1, delta1 = exchanged(1)
    beta = gamma1 / gamma0
    s_out[0] = alpha0
    s_out[1] = gamma1 / (delta1 - beta * gamma1 / alpha0)
    s_out[2] = beta


def fused_body(row_count, normal_matrix, right_side, tile_inverse, order_ids):
    block_rows, block_cols = normal_matrix.shape
    nrhs = right_side.shape[1]
    tiles, width = tile_inverse.shape[:2]
    steps = block_rows // width
    depth = row_count // 2
    f32, bf16 = jnp.float32, jnp.bfloat16
    whole = jax.ShapeDtypeStruct((nrhs, block_cols), f32)
    dma = pltpu.SemaphoreType.DMA
    vmem = pl.BlockSpec(memory_space=pltpu.VMEM)
    hbm = pl.BlockSpec(memory_space=pl.ANY)
    hh = nrhs // 2
    b = right_side.T
    u, m, w, n, scalars = pl.pallas_call(
        functools.partial(kernel, depth, width),
        out_shape=(whole, whole, whole, whole, jax.ShapeDtypeStruct((3, nrhs, width), f32)),
        in_specs=[hbm, hbm, hbm, vmem],
        out_specs=(hbm, hbm, hbm, hbm, vmem),
        scratch_shapes=[
            pltpu.VMEM((steps, width, block_cols), f32),
            pltpu.VMEM((steps, 2 * width, block_cols), bf16),
            pltpu.VMEM((tiles, width, width), f32),
            pltpu.VMEM((tiles, width, 2 * width), bf16),
            pltpu.VMEM((2 * nrhs, block_cols), bf16),
            pltpu.VMEM((4, 2 * nrhs, width), bf16),
            pltpu.VMEM((nrhs, block_cols), f32),
            pltpu.VMEM((nrhs, block_cols), f32),
            pltpu.VMEM((nrhs, block_cols), f32),
            pltpu.VMEM((2, nrhs, block_rows), f32),
            pltpu.VMEM((2, hh, block_rows), f32),
            pltpu.VMEM((2, hh, block_rows), f32),
            pltpu.VMEM((2, hh, block_rows), f32),
            pltpu.VMEM((2, hh, block_rows), f32),
            pltpu.VMEM((2, nrhs, block_cols), f32),
            pltpu.VMEM((nrhs, block_rows), f32),
            pltpu.VMEM((2 * nrhs, width), f32),
            pltpu.VMEM((2, 8, width), f32),
            pltpu.VMEM((2, 3, 8, width), f32),
            pltpu.VMEM((2 * depth - 1, 8, width), f32),
            pltpu.VMEM((2, 8, width), f32),
            pltpu.VMEM((width, width), f32),
            dma((steps,)),
            dma((2,)),
            dma((4,)),
            dma((2, steps)),
            dma((2, steps)),
            dma((2, steps)),
            dma((2, steps)),
            dma((2,)),
            dma((2,)),
            dma((2, 4)),
            dma((2, 2)),
            dma((2,)),
            dma((2,)),
            dma((1,)),
            dma((1,)),
        ],
        compiler_params=pltpu.CompilerParams(
            collective_id=0, has_side_effects=True, vmem_limit_bytes=60 * 1024 * 1024
        ),
    )(normal_matrix, tile_inverse, b, order_ids.reshape(tiles, width))
    alpha0, alpha1, beta = scalars[0, :, :1], scalars[1, :, :1], scalars[2, :, :1]
    pre = u - alpha0 * m
    sol = alpha0 * u + alpha1 * (pre + beta * u)
    res = (b - alpha0 * w) - alpha1 * ((w - alpha0 * n) + beta * w)
    return sol.T, res.T


def body(row_count, col_count, normal_matrix, right_side, tile_inverse, order_ids):
    block_rows, block_cols = normal_matrix.shape
    width = tile_inverse.shape[1]
    fits = (
        col_count == 4
        and row_count == 8
        and block_cols == 2 * block_rows
        and block_rows % width == 0
        and width == 128
        and tile_inverse.shape[0] <= width
        and right_side.shape[1] == 64
    )
    if fits:
        return fused_body(row_count, normal_matrix, right_side, tile_inverse, order_ids)
    return plain_body(normal_matrix, right_side, tile_inverse, order_ids)


def solution(mesh):
    return jax.shard_map(
        functools.partial(body, mesh.shape["row"], mesh.shape["col"]),
        mesh=mesh,
        in_specs=(P("row", "col"), P("col", None), P("col", None, None), P("col")),
        out_specs=(P("col", None), P("col", None)),
        check_vma=False,
    )
```

```python
import functools

import jax
import jax.numpy as jnp
from jax import lax
from jax.experimental import pallas as pl
from jax.experimental.pallas import tpu as pltpu
from jax.sharding import PartitionSpec as P

ITERS = 2
MESH = pl.DeviceIdType.MESH
NEAR_LAG = 3


def masked_tiles(tile_inverse, order_ids):
    count = tile_inverse.shape[0]
    width = tile_inverse.shape[1]
    order_tile = order_ids.reshape(count, width)
    same_order = order_tile[:, :, None] == order_tile[:, None, :]
    return jnp.where(same_order, tile_inverse, jnp.float32(0.0))


def apply_precond(tile_inverse, order_ids, vector):
    count = tile_inverse.shape[0]
    width = tile_inverse.shape[1]
    masked = masked_tiles(tile_inverse, order_ids)
    pieces = vector.reshape(count, width, vector.shape[1])
    result = jnp.einsum("tij,tjk->tik", masked, pieces, precision=lax.Precision.HIGHEST)
    return result.reshape(vector.shape)


def plain_body(normal_matrix, right_side, tile_inverse, order_ids):
    block_rows = normal_matrix.shape[0]

    def apply_matrix(vector):
        first_row = lax.axis_index("row") * block_rows
        gathered = lax.all_gather(vector, "col", axis=0, tiled=True)
        row_piece = lax.dynamic_slice_in_dim(gathered, first_row, block_rows, 0)
        partial_value = lax.dot_general(
            normal_matrix,
            row_piece,
            (((0,), (0,)), ((), ())),
            precision=lax.Precision.HIGHEST,
            preferred_element_type=jnp.float32,
        )
        return lax.psum(partial_value, "row")

    solution = jnp.zeros_like(right_side)
    residual = right_side
    precond_res = apply_precond(tile_inverse, order_ids, residual)
    image_res = apply_matrix(precond_res)
    image_dir = jnp.zeros_like(right_side)
    precond_dir = jnp.zeros_like(right_side)
    residual_dir = jnp.zeros_like(right_side)
    direction = jnp.zeros_like(right_side)
    gamma_prev = jnp.ones((right_side.shape[1],), jnp.float32)
    alpha_prev = jnp.ones((right_side.shape[1],), jnp.float32)
    for iteration in range(ITERS):
        gamma_now, delta_now = lax.psum(
            (jnp.sum(residual * precond_res, axis=0), jnp.sum(image_res * precond_res, axis=0)),
            "col",
        )
        precond_img = apply_precond(tile_inverse, order_ids, image_res)
        image_img = apply_matrix(precond_img)
        if iteration == 0:
            beta_ratio = jnp.zeros_like(gamma_now)
            step_size = gamma_now / delta_now
        else:
            beta_ratio = gamma_now / gamma_prev
            step_size = gamma_now / (delta_now - beta_ratio * gamma_now / alpha_prev)
        image_dir = image_img + beta_ratio * image_dir
        precond_dir = precond_img + beta_ratio * precond_dir
        residual_dir = image_res + beta_ratio * residual_dir
        direction = precond_res + beta_ratio * direction
        solution = solution + step_size * direction
        residual = residual - step_size * residual_dir
        precond_res = precond_res - step_size * precond_dir
        image_res = image_res - step_size * image_dir
        gamma_prev = gamma_now
        alpha_prev = step_size
    return (solution, residual)


def halves(value):
    high = value.astype(jnp.bfloat16)
    low = (value - high.astype(jnp.float32)).astype(jnp.bfloat16)
    return high, low


def split(value):
    return jnp.concatenate(halves(value), axis=0)


def times(left, right):
    return lax.dot_general(
        left, right, (((1,), (0,)), ((), ())), preferred_element_type=jnp.float32
    )


def times_transposed(left, right):
    return lax.dot_general(
        left, right, (((1,), (1,)), ((), ())), preferred_element_type=jnp.float32
    )


def fold(product, rows, columns):
    both = product[:rows] + product[rows:]
    return both[:, :columns] + both[:, columns:]


def kernel(
    depth, width,
    a_ref, tile_ref, b_ref, ids_ref,
    sol_ref, res_ref,
    a_buf, a_split, tile_buf, tile_split, v_split, v_minus, m_split, b_buf, u_buf, m_buf,
    part, near, half, far, done, image, acc,
    sums, dot_own, dot_in, delta_own, delta_fill, delta_in, ids_buf,
    a_sem, in_sem, near_sem, far_sem, line_sem, side_sem,
    near_send, far_send, fan_send, relay_send, dot_send, dot_recv, delta_send, delta_recv,
):
    my_row, my_col = lax.axis_index("row"), lax.axis_index("col")
    place, lane = my_row // 2, lax.rem(my_row, 2)
    core = lax.rem(my_col, 2)
    partner = my_col + 1 - 2 * core
    across = lax.rem(my_col + 2, 4)
    side = my_row + 1 - 2 * lane
    owner = place == my_col
    owner_chip = place // 2 == my_col // 2
    helper = jnp.logical_and(owner_chip, jnp.logical_not(owner))
    others = jnp.logical_not(owner)
    above, below = place < depth - 1, place > 0
    nrhs, block_cols = b_buf.shape
    block_rows = acc.shape[1]
    hh = nrhs // 2
    tiles = block_cols // width
    steps = block_rows // width
    mine = pl.ds(pl.multiple_of(core * hh, hh), hh)
    other = pl.ds(pl.multiple_of((1 - core) * hh, hh), hh)

    def fetch(i):
        return pltpu.make_async_copy(a_ref.at[pl.ds(i * width, width)], a_buf.at[i], a_sem.at[i])

    first_tiles = tiles // 2
    pieces = (pl.ds(0, first_tiles), pl.ds(first_tiles, tiles - first_tiles))

    def fetch_tiles(k):
        return pltpu.make_async_copy(tile_ref.at[pieces[k]], tile_buf.at[pieces[k]], in_sem.at[k])

    fetch_b = pltpu.make_async_copy(b_ref, b_buf, in_sem.at[2])
    fetch_tiles(0).start()
    fetch_tiles(1).start()
    fetch_b.start()

    barrier = pltpu.get_barrier_semaphore()

    def greet(row, col):
        pl.semaphore_signal(barrier, inc=1, device_id=(row, col), device_id_type=MESH)

    for shift in range(1, 4):
        greet(my_row, lax.rem(my_col + shift, 4))
    greet(side, my_col)
    greet(2 * my_col + 1 - lane, my_col)

    @pl.when(others)
    def _():
        greet(2 * my_col + lane, my_col)

    @pl.when(place > my_col)
    def _():
        greet(my_row - 2, my_col)

    @pl.when(place < my_col)
    def _():
        greet(my_row + 2, my_col)

    @pl.when(jnp.logical_or(place == my_col + 1, place == my_col - 1))
    def _():
        greet(2 * my_col + lane, partner)

    @pl.when(owner)
    def _():
        greet(side, partner)

    goes_up = jnp.logical_and(place >= my_col, above)
    goes_down = jnp.logical_and(place <= my_col, below)

    def one(flag):
        return jnp.where(flag, 1, 0)

    def meet():
        awaited = 4 + one(goes_up) + one(goes_down)
        awaited += jnp.where(helper, 1 + one(above) + one(below), 0)
        awaited += jnp.where(owner, 2 * depth - 1, 0)
        pl.semaphore_wait(barrier, awaited)

    def lanes_at(t):
        return pl.ds(pl.multiple_of(t * width, width), width)

    def cut(q):
        return pl.ds(q * width, width)

    def lanes_of(block, q):
        return lanes_at(block * steps + q)

    def near_chunk(turn, q):
        return pltpu.make_async_remote_copy(
            src_ref=part.at[turn, other, cut(q)], dst_ref=near.at[turn, :, cut(q)],
            send_sem=near_send.at[turn], recv_sem=near_sem.at[turn, q],
            device_id=(my_row, partner), device_id_type=MESH,
        )

    def far_chunk(turn, q):
        return pltpu.make_async_remote_copy(
            src_ref=half.at[turn, :, cut(q)], dst_ref=far.at[turn, :, cut(q)],
            send_sem=far_send.at[turn], recv_sem=far_sem.at[turn, q],
            device_id=(my_row, across), device_id_type=MESH,
        )

    def fan_chunk(turn, q, way, row, sem):
        return pltpu.make_async_remote_copy(
            src_ref=done.at[turn, :, cut(q)], dst_ref=image.at[turn, mine, lanes_of(lane, q)],
            send_sem=fan_send.at[turn, way], recv_sem=sem.at[turn, q],
            device_id=(row, place), device_id_type=MESH,
        )

    def relay_chunk(turn, q, way, row, sem):
        return pltpu.make_async_remote_copy(
            src_ref=image.at[turn, :, lanes_of(lane, q)], dst_ref=image.at[turn, :, lanes_of(lane, q)],
            send_sem=relay_send.at[turn, way], recv_sem=sem.at[turn, q],
            device_id=(row, my_col), device_id_type=MESH,
        )

    def stage1(turn, q):
        near_chunk(turn, q).wait_recv()
        half[turn, :, cut(q)] = part[turn, mine, cut(q)] + near[turn, :, cut(q)]

        @pl.when(jnp.logical_not(owner_chip))
        def _():
            far_chunk(turn, q).start()

    def stage2(turn, q):
        @pl.when(owner_chip)
        def _():
            far_chunk(turn, q).wait_recv()
            total = half[turn, :, cut(q)] + far[turn, :, cut(q)]
            done[turn, :, cut(q)] = total

            @pl.when(above)
            def _():
                fan_chunk(turn, q, 0, my_row + 2, line_sem).start()

            @pl.when(below)
            def _():
                fan_chunk(turn, q, 1, my_row - 2, line_sem).start()

            fan_chunk(turn, q, 2, side, side_sem).start()

            @pl.when(helper)
            def _():
                fan_chunk(turn, q, 3, my_row, line_sem).start()

            @pl.when(owner)
            def _():
                image[turn, mine, lanes_of(lane, q)] = total

    def own(turn, q):
        @pl.when(owner)
        def _():
            pltpu.make_async_remote_copy(
                src_ref=done.at[turn, :, cut(q)], dst_ref=image.at[turn, other, lanes_of(lane, q)],
                send_sem=fan_send.at[turn, 3], recv_sem=line_sem.at[turn, q],
                device_id=(my_row, partner), device_id_type=MESH,
            ).wait_recv()

        @pl.when(others)
        def _():
            relay_chunk(turn, q, 0, my_row, line_sem).wait_recv()

            @pl.when(goes_up)
            def _():
                relay_chunk(turn, q, 0, my_row + 2, line_sem).start()

            @pl.when(goes_down)
            def _():
                relay_chunk(turn, q, 0, my_row - 2, line_sem).start()

            relay_chunk(turn, q, 1, side, side_sem).start()

    def beside(turn, q):
        pltpu.make_async_remote_copy(
            src_ref=image.at[turn, :, lanes_of(1 - lane, q)], dst_ref=image.at[turn, :, lanes_of(1 - lane, q)],
            send_sem=relay_send.at[turn, 1], recv_sem=side_sem.at[turn, q],
            device_id=(side, my_col), device_id_type=MESH,
        ).wait_recv()

    def finish(turn):
        near_all = pltpu.make_async_remote_copy(
            src_ref=part.at[turn, other], dst_ref=near.at[turn],
            send_sem=near_send.at[turn], recv_sem=near_sem.at[turn, 0],
            device_id=(my_row, partner), device_id_type=MESH,
        )
        near_all.wait_send()

        def fan_all(way):
            return pltpu.make_async_remote_copy(
                src_ref=done.at[turn], dst_ref=far.at[turn],
                send_sem=fan_send.at[turn, way], recv_sem=line_sem.at[turn, 0],
                device_id=(side, my_col), device_id_type=MESH,
            )

        def relay_all(way):
            return pltpu.make_async_remote_copy(
                src_ref=part.at[turn], dst_ref=part.at[turn],
                send_sem=relay_send.at[turn, way], recv_sem=line_sem.at[turn, 0],
                device_id=(side, my_col), device_id_type=MESH,
            )

        @pl.when(jnp.logical_not(owner_chip))
        def _():
            pltpu.make_async_remote_copy(
                src_ref=half.at[turn], dst_ref=far.at[turn],
                send_sem=far_send.at[turn], recv_sem=far_sem.at[turn, 0],
                device_id=(my_row, across), device_id_type=MESH,
            ).wait_send()

        @pl.when(owner_chip)
        def _():
            @pl.when(above)
            def _():
                fan_all(0).wait_send()

            @pl.when(below)
            def _():
                fan_all(1).wait_send()

            fan_all(2).wait_send()

            @pl.when(helper)
            def _():
                fan_all(3).wait_send()

        @pl.when(others)
        def _():
            @pl.when(jnp.logical_or(goes_up, goes_down))
            def _():
                relay_all(0).wait_send()

            relay_all(1).wait_send()

    def dot_row():
        return jnp.sum(sums[...].T, axis=0, keepdims=True)

    def exchange(turn, row):
        dot_own[turn] = jnp.broadcast_to(row, dot_own.shape[1:])
        for shift in (2, 1, 3):
            pltpu.make_async_remote_copy(
                src_ref=dot_own.at[turn], dst_ref=dot_in.at[turn, shift - 1],
                send_sem=dot_send.at[turn], recv_sem=dot_recv.at[turn],
                device_id=(my_row, lax.rem(my_col + shift, 4)), device_id_type=MESH,
            ).start()

    def exchanged(turn):
        pltpu.make_async_remote_copy(
            src_ref=dot_in.at[turn], dst_ref=dot_in.at[turn],
            send_sem=dot_send.at[turn], recv_sem=dot_recv.at[turn],
            device_id=(my_row, partner), device_id_type=MESH,
        ).wait()
        total = (dot_own[turn] + dot_in[turn, 1]) + (dot_in[turn, 0] + dot_in[turn, 2])
        across_lanes = jnp.broadcast_to(total[0:1], (2 * nrhs, width)).T
        return across_lanes[:nrhs], across_lanes[nrhs:]

    ids_buf[...] = jnp.zeros_like(ids_buf)
    ids_buf[0:tiles] = ids_ref[...].astype(jnp.float32)
    ids_across = ids_buf[...].T
    fetch(0).start()
    fetch_tiles(0).wait()
    fetch(1).start()
    fetch(2).start()
    for t in range(tiles):
        if t == first_tiles:
            fetch_tiles(1).wait()
            fetch_b.wait()
            for i in range(3, steps):
                fetch(i).start()
        same = ids_across[:, t : t + 1] == ids_buf[t : t + 1]
        tile_split[t] = jnp.concatenate(halves(jnp.where(same, tile_buf[t], 0.0)), axis=1)
    gamma = jnp.zeros((nrhs, width), jnp.float32)
    for t in range(tiles):
        value = b_buf[:, cut(t)]
        product = fold(times(split(value), tile_split[t]), nrhs, width)
        u_buf[:, cut(t)] = product
        parts = split(product)
        v_split[:, cut(t)] = parts
        v_minus[:, cut(t)] = -parts
        gamma += value * product
    sums[:nrhs] = gamma
    sums[nrhs:] = jnp.zeros_like(gamma)

    met = False
    halved = 0
    for begin in [0] + list(range(1, steps, 2)):
        group = range(begin, min(begin + 2, steps)) if begin else range(1)
        for q in group:
            fetch(q).wait()
        for q in group:
            a_split[q] = split(a_buf[q])
            high = times_transposed(v_split[...], a_split[q, :width])
            minus_low = times_transposed(v_minus[...], a_split[q, width:])
            part[0, :, cut(q)] = (high[:nrhs] - minus_low[:nrhs]) + (high[nrhs:] - minus_low[nrhs:])
        if not met:
            meet()
            met = True
        for q in group:
            near_chunk(0, q).start()
        while halved <= group[-1] - NEAR_LAG:
            stage1(0, halved)
            halved += 1
    for q in range(halved, steps):
        stage1(0, q)

    acc[...] = jnp.zeros_like(acc)

    def take(block, q, slot):
        lanes = lanes_of(block, q)
        value = image[0, :, lanes]
        product = fold(times(split(value), tile_split[block * steps + q]), nrhs, width)
        m_buf[:, lanes] = product
        m_split[slot] = split(product)
        sums[nrhs:] += value * u_buf[:, lanes]
        return slot, lanes

    def update(taken, i):
        product = None
        for slot, lanes in taken:
            term = times_transposed(m_split[slot], a_split[i, :, lanes])
            product = term if product is None else product + term
        return acc[:, cut(i)] + fold(product, nrhs, width)

    for q in range(steps):
        stage2(0, q)
    arrivals = [(lane, q) for q in range(steps)] + [(1 - lane, q) for q in range(steps)]
    taken = []
    for begin in range(0, 2 * steps, 2):
        for k in (begin, begin + 1):
            if k < steps:
                own(0, k)
            else:
                beside(0, k - steps)
        if taken:
            for i in range(steps):
                acc[:, cut(i)] = update(taken, i)
        taken = [take(*arrivals[k], k % 4) for k in (begin, begin + 1)]
    for i in range(steps):
        part[1, :, cut(i)] = update(taken, i)
    for i in range(steps):
        near_chunk(1, i).start()
    exchange(0, dot_row())
    for q in range(steps):
        stage1(1, q)
    gamma0, delta0 = exchanged(0)
    alpha0 = gamma0 / delta0
    gamma = jnp.zeros((nrhs, width), jnp.float32)
    for t in range(tiles):
        lanes = cut(t)
        res = b_buf[:, lanes] - alpha0 * image[0, :, lanes]
        pre = u_buf[:, lanes] - alpha0 * m_buf[:, lanes]
        gamma += res * pre
    sums[:nrhs] = gamma
    sums[nrhs:] = jnp.zeros_like(gamma)
    exchange(1, dot_row())

    rows = 2 * depth

    def slot_of(origin, target):
        return lax.rem(origin - target + rows, rows)

    def deltas():
        @pl.when(owner)
        def _():
            delta_own[...] = jnp.broadcast_to(dot_row(), delta_own.shape)
            delta_in[0] = delta_own[...]
            for i in range(rows):
                target = lax.rem(my_row + i, rows)
                for shift in range(4):
                    if i or shift:
                        pltpu.make_async_remote_copy(
                            src_ref=delta_own, dst_ref=delta_in.at[slot_of(my_row, target)],
                            send_sem=delta_send.at[0], recv_sem=delta_recv.at[0],
                            device_id=(target, lax.rem(my_col + shift, 4)), device_id_type=MESH,
                        ).start()

    for q in range(steps):
        stage2(1, q)
    for q in range(steps):
        own(1, q)

        @pl.when(owner)
        def _():
            lanes = lanes_of(lane, q)
            img = image[0, :, lanes] - alpha0 * image[1, :, lanes]
            sums[nrhs:] += img * (u_buf[:, lanes] - alpha0 * m_buf[:, lanes])

    deltas()
    for q in range(steps):
        beside(1, q)

    def delta_copy(slots):
        return pltpu.make_async_remote_copy(
            src_ref=slots, dst_ref=slots, send_sem=delta_send.at[0], recv_sem=delta_recv.at[0],
            device_id=(side, my_col), device_id_type=MESH,
        )

    finish(0)
    finish(1)

    @pl.when(owner)
    def _():
        delta_copy(delta_fill).wait_send()
        delta_copy(delta_in.at[pl.ds(1, rows - 1)]).wait_recv()

    @pl.when(others)
    def _():
        delta_copy(delta_in).wait_recv()

    gamma1 = exchanged(1)[0]
    total = delta_in[slot_of(0, my_row)]
    for origin in range(1, rows):
        total = total + delta_in[slot_of(origin, my_row)]
    delta1 = jnp.broadcast_to(total[0:1], (2 * nrhs, width)).T[nrhs:]
    beta = gamma1 / gamma0
    alpha1 = gamma1 / (delta1 - beta * gamma1 / alpha0)
    for t in range(tiles):
        lanes = cut(t)
        u, w = u_buf[:, lanes], image[0, :, lanes]
        pre = u - alpha0 * m_buf[:, lanes]
        img = w - alpha0 * image[1, :, lanes]
        sol_ref[:, lanes] = alpha0 * u + alpha1 * (pre + beta * u)
        res_ref[:, lanes] = (b_buf[:, lanes] - alpha0 * w) - alpha1 * (img + beta * w)


def fused_body(row_count, normal_matrix, right_side, tile_inverse, order_ids):
    block_rows, block_cols = normal_matrix.shape
    nrhs = right_side.shape[1]
    tiles, width = tile_inverse.shape[:2]
    steps = block_rows // width
    depth = row_count // 2
    f32, bf16 = jnp.float32, jnp.bfloat16
    whole = jax.ShapeDtypeStruct((nrhs, block_cols), f32)
    dma = pltpu.SemaphoreType.DMA
    vmem = pl.BlockSpec(memory_space=pltpu.VMEM)
    hbm = pl.BlockSpec(memory_space=pltpu.HBM)
    hh = nrhs // 2
    sol, res = pl.pallas_call(
        functools.partial(kernel, depth, width),
        out_shape=(whole, whole),
        in_specs=[hbm, hbm, hbm, vmem],
        out_specs=(vmem, vmem),
        scratch_shapes=[
            pltpu.VMEM((steps, width, block_cols), f32),
            pltpu.VMEM((steps, 2 * width, block_cols), bf16),
            pltpu.VMEM((tiles, width, width), f32),
            pltpu.VMEM((tiles, width, 2 * width), bf16),
            pltpu.VMEM((2 * nrhs, block_cols), bf16),
            pltpu.VMEM((2 * nrhs, block_cols), bf16),
            pltpu.VMEM((4, 2 * nrhs, width), bf16),
            pltpu.VMEM((nrhs, block_cols), f32),
            pltpu.VMEM((nrhs, block_cols), f32),
            pltpu.VMEM((nrhs, block_cols), f32),
            pltpu.VMEM((2, nrhs, block_rows), f32),
            pltpu.VMEM((2, hh, block_rows), f32),
            pltpu.VMEM((2, hh, block_rows), f32),
            pltpu.VMEM((2, hh, block_rows), f32),
            pltpu.VMEM((2, hh, block_rows), f32),
            pltpu.VMEM((2, nrhs, block_cols), f32),
            pltpu.VMEM((nrhs, block_rows), f32),
            pltpu.VMEM((2 * nrhs, width), f32),
            pltpu.VMEM((2, 8, width), f32),
            pltpu.VMEM((2, 3, 8, width), f32),
            pltpu.VMEM((8, width), f32),
            pltpu.VMEM((8 * depth - 1, 8, width), f32),
            pltpu.VMEM((2 * depth, 8, width), f32),
            pltpu.VMEM((width, width), f32),
            dma((steps,)),
            dma((3,)),
            dma((2, steps)),
            dma((2, steps)),
            dma((2, steps)),
            dma((2, steps)),
            dma((2,)),
            dma((2,)),
            dma((2, 4)),
            dma((2, 2)),
            dma((2,)),
            dma((2,)),
            dma((1,)),
            dma((1,)),
        ],
        compiler_params=pltpu.CompilerParams(
            collective_id=0, has_side_effects=True, vmem_limit_bytes=53500 * 1024
        ),
    )(normal_matrix, tile_inverse, right_side.T, order_ids.reshape(tiles, width))
    return sol.T, res.T


def body(row_count, col_count, normal_matrix, right_side, tile_inverse, order_ids):
    block_rows, block_cols = normal_matrix.shape
    width = tile_inverse.shape[1]
    fits = (
        col_count == 4
        and row_count == 8
        and block_cols == 2 * block_rows
        and block_rows % width == 0
        and width == 128
        and tile_inverse.shape[0] <= width
        and right_side.shape[1] == 64
    )
    if fits:
        return fused_body(row_count, normal_matrix, right_side, tile_inverse, order_ids)
    return plain_body(normal_matrix, right_side, tile_inverse, order_ids)


def solution(mesh):
    return jax.shard_map(
        functools.partial(body, mesh.shape["row"], mesh.shape["col"]),
        mesh=mesh,
        in_specs=(P("row", "col"), P("col", None), P("col", None, None), P("col")),
        out_specs=(P("col", None), P("col", None)),
        check_vma=False,
    )
```

```python
import functools

import jax
import jax.numpy as jnp
from jax import lax
from jax.experimental import pallas as pl
from jax.experimental.pallas import tpu as pltpu
from jax.sharding import PartitionSpec as P

ITERS = 2
MESH = pl.DeviceIdType.MESH
NEAR_LAG = 2
FETCHES = ((0, 1), (1, 2), (3, 2), (5, 2), (7, 2))


def masked_tiles(tile_inverse, order_ids):
    count = tile_inverse.shape[0]
    width = tile_inverse.shape[1]
    order_tile = order_ids.reshape(count, width)
    same_order = order_tile[:, :, None] == order_tile[:, None, :]
    return jnp.where(same_order, tile_inverse, jnp.float32(0.0))


def apply_precond(tile_inverse, order_ids, vector):
    count = tile_inverse.shape[0]
    width = tile_inverse.shape[1]
    masked = masked_tiles(tile_inverse, order_ids)
    pieces = vector.reshape(count, width, vector.shape[1])
    result = jnp.einsum("tij,tjk->tik", masked, pieces, precision=lax.Precision.HIGHEST)
    return result.reshape(vector.shape)


def plain_body(normal_matrix, right_side, tile_inverse, order_ids):
    block_rows = normal_matrix.shape[0]

    def apply_matrix(vector):
        first_row = lax.axis_index("row") * block_rows
        gathered = lax.all_gather(vector, "col", axis=0, tiled=True)
        row_piece = lax.dynamic_slice_in_dim(gathered, first_row, block_rows, 0)
        partial_value = lax.dot_general(
            normal_matrix,
            row_piece,
            (((0,), (0,)), ((), ())),
            precision=lax.Precision.HIGHEST,
            preferred_element_type=jnp.float32,
        )
        return lax.psum(partial_value, "row")

    solution = jnp.zeros_like(right_side)
    residual = right_side
    precond_res = apply_precond(tile_inverse, order_ids, residual)
    image_res = apply_matrix(precond_res)
    image_dir = jnp.zeros_like(right_side)
    precond_dir = jnp.zeros_like(right_side)
    residual_dir = jnp.zeros_like(right_side)
    direction = jnp.zeros_like(right_side)
    gamma_prev = jnp.ones((right_side.shape[1],), jnp.float32)
    alpha_prev = jnp.ones((right_side.shape[1],), jnp.float32)
    for iteration in range(ITERS):
        gamma_now, delta_now = lax.psum(
            (jnp.sum(residual * precond_res, axis=0), jnp.sum(image_res * precond_res, axis=0)),
            "col",
        )
        precond_img = apply_precond(tile_inverse, order_ids, image_res)
        image_img = apply_matrix(precond_img)
        if iteration == 0:
            beta_ratio = jnp.zeros_like(gamma_now)
            step_size = gamma_now / delta_now
        else:
            beta_ratio = gamma_now / gamma_prev
            step_size = gamma_now / (delta_now - beta_ratio * gamma_now / alpha_prev)
        image_dir = image_img + beta_ratio * image_dir
        precond_dir = precond_img + beta_ratio * precond_dir
        residual_dir = image_res + beta_ratio * residual_dir
        direction = precond_res + beta_ratio * direction
        solution = solution + step_size * direction
        residual = residual - step_size * residual_dir
        precond_res = precond_res - step_size * precond_dir
        image_res = image_res - step_size * image_dir
        gamma_prev = gamma_now
        alpha_prev = step_size
    return (solution, residual)


def halves(value):
    high = value.astype(jnp.bfloat16)
    low = (value - high.astype(jnp.float32)).astype(jnp.bfloat16)
    return high, low


def split(value):
    return jnp.concatenate(halves(value), axis=0)


def times(left, right):
    return lax.dot_general(
        left, right, (((1,), (0,)), ((), ())), preferred_element_type=jnp.float32
    )


def times_transposed(left, right):
    return lax.dot_general(
        left, right, (((1,), (1,)), ((), ())), preferred_element_type=jnp.float32
    )


def fold(product, rows, columns):
    both = product[:rows] + product[rows:]
    return both[:, :columns] + both[:, columns:]


def kernel(
    depth, width,
    a_ref, tile_ref, b_ref, ids_ref,
    sol_ref, res_ref,
    a_buf, a_split, tile_buf, tile_split, v_split, v_minus, m_split, b_buf, u_buf, m_buf,
    part, near, half, far, done, hop, image, acc,
    sums, dot_own, dot_in, delta_own, delta_fill, delta_in, ids_buf,
    a_sem, in_sem, near_sem, far_sem, line_sem, side_sem, hop_sem,
    near_send, far_send, hop_send, slant_send, fan_send, relay_send, dot_send, dot_recv, delta_send, delta_recv,
):
    my_row, my_col = lax.axis_index("row"), lax.axis_index("col")
    place, lane = my_row // 2, lax.rem(my_row, 2)
    core = lax.rem(my_col, 2)
    partner = my_col + 1 - 2 * core
    across = lax.rem(my_col + 2, 4)
    side = my_row + 1 - 2 * lane
    owner = place == my_col
    owner_chip = place // 2 == my_col // 2
    helper = jnp.logical_and(owner_chip, jnp.logical_not(owner))
    others = jnp.logical_not(owner)
    above, below = place < depth - 1, place > 0
    nrhs, block_cols = b_buf.shape
    block_rows = acc.shape[1]
    hh = nrhs // 2
    tiles = block_cols // width
    steps = block_rows // width
    mine = pl.ds(pl.multiple_of(core * hh, hh), hh)
    other = pl.ds(pl.multiple_of((1 - core) * hh, hh), hh)

    def fetch(k):
        begin, count = FETCHES[k]
        return pltpu.make_async_copy(
            a_ref.at[pl.ds(begin * width, count * width)],
            a_buf.at[pl.ds(begin * width, count * width)], a_sem.at[k],
        )

    first_tiles = tiles // 2
    pieces = (pl.ds(0, first_tiles), pl.ds(first_tiles, tiles - first_tiles))

    def fetch_tiles(k):
        return pltpu.make_async_copy(tile_ref.at[pieces[k]], tile_buf.at[pieces[k]], in_sem.at[k])

    fetch_b = pltpu.make_async_copy(b_ref, b_buf, in_sem.at[2])
    fetch_tiles(0).start()
    fetch_tiles(1).start()
    fetch_b.start()

    barrier = pltpu.get_barrier_semaphore()

    def greet(row, col):
        pl.semaphore_signal(barrier, inc=1, device_id=(row, col), device_id_type=MESH)

    for shift in range(1, 4):
        greet(my_row, lax.rem(my_col + shift, 4))
    greet(side, my_col)

    last = depth - 1
    at_end = jnp.logical_or(place == 0, place == last)
    carrier = jnp.logical_and(at_end, owner_chip)
    origin = jnp.logical_and(at_end, jnp.logical_not(owner_chip))
    far_end = 2 * (last - place) + lane
    carried = jnp.logical_and(at_end, my_col == last - place)
    from_line = jnp.logical_and(others, jnp.logical_not(carried))
    slanted = jnp.logical_and(carrier, core == 0)

    @pl.when(jnp.logical_and(from_line, place > my_col))
    def _():
        greet(my_row - 2, my_col)

    @pl.when(jnp.logical_and(from_line, place < my_col))
    def _():
        greet(my_row + 2, my_col)

    @pl.when(jnp.logical_or(place == my_col + 1, place == my_col - 1))
    def _():
        greet(2 * my_col + lane, partner)

    @pl.when(owner)
    def _():
        greet(side, partner)

    @pl.when(carrier)
    def _():
        greet(far_end, my_col)

    @pl.when(carried)
    def _():
        greet(side, 2 * (place // 2))

    goes_up = jnp.logical_and(jnp.logical_and(place >= my_col, above), my_col + last - 1 != place)
    goes_down = jnp.logical_and(jnp.logical_and(place <= my_col, below), my_col - last + 1 != place)

    def one(flag):
        return jnp.where(flag, 1, 0)

    def meet():
        awaited = 4 + one(goes_up) + one(goes_down)
        awaited += jnp.where(helper, 1 + one(above) + one(below), 0)
        awaited += one(origin) + one(slanted)
        pl.semaphore_wait(barrier, awaited)

    def lanes_at(t):
        return pl.ds(pl.multiple_of(t * width, width), width)

    def cut(q):
        return pl.ds(q * width, width)

    def lanes_of(block, q):
        return lanes_at(block * steps + q)

    def near_group(turn, k):
        begin, count = FETCHES[k]
        lanes = pl.ds(begin * width, count * width)
        return pltpu.make_async_remote_copy(
            src_ref=part.at[turn, other, lanes], dst_ref=near.at[turn, :, lanes],
            send_sem=near_send.at[turn], recv_sem=near_sem.at[turn, k],
            device_id=(my_row, partner), device_id_type=MESH,
        )

    def far_chunk(turn, q):
        return pltpu.make_async_remote_copy(
            src_ref=half.at[turn, :, cut(q)], dst_ref=far.at[turn, :, cut(q)],
            send_sem=far_send.at[turn], recv_sem=far_sem.at[turn, q],
            device_id=(my_row, across), device_id_type=MESH,
        )

    def fan_chunk(turn, q, way, row, sem):
        return pltpu.make_async_remote_copy(
            src_ref=done.at[turn, :, cut(q)], dst_ref=image.at[turn, mine, lanes_of(lane, q)],
            send_sem=fan_send.at[turn, way], recv_sem=sem.at[turn, q],
            device_id=(row, place), device_id_type=MESH,
        )

    def relay_chunk(turn, q, way, row, sem):
        return pltpu.make_async_remote_copy(
            src_ref=image.at[turn, :, lanes_of(lane, q)], dst_ref=image.at[turn, :, lanes_of(lane, q)],
            send_sem=relay_send.at[turn, way], recv_sem=sem.at[turn, q],
            device_id=(row, my_col), device_id_type=MESH,
        )

    def hop_chunk(turn, q):
        return pltpu.make_async_remote_copy(
            src_ref=done.at[turn, :, cut(q)], dst_ref=hop.at[turn, :, cut(q)],
            send_sem=hop_send.at[turn], recv_sem=hop_sem.at[turn, q],
            device_id=(far_end, my_col), device_id_type=MESH,
        )

    def cross_chunk(turn, q):
        return pltpu.make_async_remote_copy(
            src_ref=hop.at[turn, :, cut(q)], dst_ref=image.at[turn, mine, lanes_of(lane, q)],
            send_sem=hop_send.at[turn], recv_sem=line_sem.at[turn, q],
            device_id=(my_row, last - place), device_id_type=MESH,
        )

    def slant_chunk(turn, q):
        return pltpu.make_async_remote_copy(
            src_ref=hop.at[turn, :, cut(q)], dst_ref=image.at[turn, mine, lanes_of(lane, q)],
            send_sem=slant_send.at[turn], recv_sem=side_sem.at[turn, q],
            device_id=(side, last - place), device_id_type=MESH,
        )

    def half_chunk(turn, q):
        rows_lanes = (turn, pl.ds(hh, hh), lanes_of(lane, q))
        return pltpu.make_async_remote_copy(
            src_ref=image.at[rows_lanes], dst_ref=image.at[rows_lanes],
            send_sem=relay_send.at[turn, 1], recv_sem=side_sem.at[turn, q],
            device_id=(side, my_col), device_id_type=MESH,
        )

    sends_far = jnp.logical_or(at_end, jnp.logical_not(owner_chip))
    takes_far = jnp.logical_or(at_end, owner_chip)

    def stage1(turn, k):
        near_group(turn, k).wait_recv()
        begin, count = FETCHES[k]
        for q in range(begin, begin + count):
            half[turn, :, cut(q)] = part[turn, mine, cut(q)] + near[turn, :, cut(q)]

        @pl.when(sends_far)
        def _():
            for q in range(begin, begin + count):
                far_chunk(turn, q).start()

    def carry(turn, q):
        @pl.when(carrier)
        def _():
            hop_chunk(turn, q).wait_recv()
            cross_chunk(turn, q).start()

            @pl.when(core == 0)
            def _():
                slant_chunk(turn, q).start()

    def stage2(turn, q):
        @pl.when(takes_far)
        def _():
            far_chunk(turn, q).wait_recv()
            done[turn, :, cut(q)] = half[turn, :, cut(q)] + far[turn, :, cut(q)]

        @pl.when(origin)
        def _():
            hop_chunk(turn, q).start()

        @pl.when(owner_chip)
        def _():
            @pl.when(above)
            def _():
                fan_chunk(turn, q, 0, my_row + 2, line_sem).start()

            @pl.when(below)
            def _():
                fan_chunk(turn, q, 1, my_row - 2, line_sem).start()

            fan_chunk(turn, q, 2, side, side_sem).start()

            @pl.when(helper)
            def _():
                fan_chunk(turn, q, 3, my_row, line_sem).start()

            @pl.when(owner)
            def _():
                image[turn, mine, lanes_of(lane, q)] = done[turn, :, cut(q)]

    def own(turn, q):
        @pl.when(owner)
        def _():
            pltpu.make_async_remote_copy(
                src_ref=done.at[turn, :, cut(q)], dst_ref=image.at[turn, other, lanes_of(lane, q)],
                send_sem=fan_send.at[turn, 3], recv_sem=line_sem.at[turn, q],
                device_id=(my_row, partner), device_id_type=MESH,
            ).wait_recv()

        @pl.when(others)
        def _():
            relay_chunk(turn, q, 0, my_row, line_sem).wait_recv()

            @pl.when(goes_up)
            def _():
                relay_chunk(turn, q, 0, my_row + 2, line_sem).start()

            @pl.when(goes_down)
            def _():
                relay_chunk(turn, q, 0, my_row - 2, line_sem).start()

            @pl.when(from_line)
            def _():
                relay_chunk(turn, q, 1, side, side_sem).start()

            @pl.when(carried)
            def _():
                half_chunk(turn, q).start()

    def beside(turn, q):
        pltpu.make_async_remote_copy(
            src_ref=image.at[turn, :, lanes_of(1 - lane, q)], dst_ref=image.at[turn, :, lanes_of(1 - lane, q)],
            send_sem=relay_send.at[turn, 1], recv_sem=side_sem.at[turn, q],
            device_id=(side, my_col), device_id_type=MESH,
        ).wait_recv()

    def finish(turn):
        near_all = pltpu.make_async_remote_copy(
            src_ref=part.at[turn, other], dst_ref=near.at[turn],
            send_sem=near_send.at[turn], recv_sem=near_sem.at[turn, 0],
            device_id=(my_row, partner), device_id_type=MESH,
        )
        near_all.wait_send()

        def fan_all(way):
            return pltpu.make_async_remote_copy(
                src_ref=done.at[turn], dst_ref=far.at[turn],
                send_sem=fan_send.at[turn, way], recv_sem=line_sem.at[turn, 0],
                device_id=(side, my_col), device_id_type=MESH,
            )

        def relay_all(way):
            return pltpu.make_async_remote_copy(
                src_ref=part.at[turn], dst_ref=part.at[turn],
                send_sem=relay_send.at[turn, way], recv_sem=line_sem.at[turn, 0],
                device_id=(side, my_col), device_id_type=MESH,
            )

        @pl.when(at_end)
        def _():
            pltpu.make_async_remote_copy(
                src_ref=hop.at[turn], dst_ref=hop.at[turn],
                send_sem=hop_send.at[turn], recv_sem=hop_sem.at[turn, 0],
                device_id=(far_end, my_col), device_id_type=MESH,
            ).wait_send()

        @pl.when(sends_far)
        def _():
            pltpu.make_async_remote_copy(
                src_ref=half.at[turn], dst_ref=far.at[turn],
                send_sem=far_send.at[turn], recv_sem=far_sem.at[turn, 0],
                device_id=(my_row, across), device_id_type=MESH,
            ).wait_send()

        @pl.when(owner_chip)
        def _():
            @pl.when(above)
            def _():
                fan_all(0).wait_send()

            @pl.when(below)
            def _():
                fan_all(1).wait_send()

            fan_all(2).wait_send()

            @pl.when(helper)
            def _():
                fan_all(3).wait_send()

        @pl.when(others)
        def _():
            @pl.when(jnp.logical_or(goes_up, goes_down))
            def _():
                relay_all(0).wait_send()

            @pl.when(from_line)
            def _():
                relay_all(1).wait_send()

        @pl.when(carried)
        def _():
            pltpu.make_async_remote_copy(
                src_ref=half.at[turn], dst_ref=half.at[turn],
                send_sem=relay_send.at[turn, 1], recv_sem=side_sem.at[turn, 0],
                device_id=(side, my_col), device_id_type=MESH,
            ).wait_send()

        @pl.when(slanted)
        def _():
            pltpu.make_async_remote_copy(
                src_ref=hop.at[turn], dst_ref=hop.at[turn],
                send_sem=slant_send.at[turn], recv_sem=hop_sem.at[turn, 0],
                device_id=(side, my_col), device_id_type=MESH,
            ).wait_send()

    def dot_row():
        return jnp.sum(sums[...].T, axis=0, keepdims=True)

    def exchange(turn, row):
        dot_own[turn] = jnp.broadcast_to(row, dot_own.shape[1:])
        for shift in (2, 1, 3):
            pltpu.make_async_remote_copy(
                src_ref=dot_own.at[turn], dst_ref=dot_in.at[turn, shift - 1],
                send_sem=dot_send.at[turn], recv_sem=dot_recv.at[turn],
                device_id=(my_row, lax.rem(my_col + shift, 4)), device_id_type=MESH,
            ).start()

    def exchanged(turn):
        pltpu.make_async_remote_copy(
            src_ref=dot_in.at[turn], dst_ref=dot_in.at[turn],
            send_sem=dot_send.at[turn], recv_sem=dot_recv.at[turn],
            device_id=(my_row, partner), device_id_type=MESH,
        ).wait()
        total = (dot_own[turn] + dot_in[turn, 1]) + (dot_in[turn, 0] + dot_in[turn, 2])
        across_lanes = jnp.broadcast_to(total[0:1], (2 * nrhs, width)).T
        return across_lanes[:nrhs], across_lanes[nrhs:]

    ids_buf[...] = jnp.zeros_like(ids_buf)
    ids_buf[0:tiles] = ids_ref[...].astype(jnp.float32)
    ids_across = ids_buf[...].T
    fetch(0).start()
    fetch_tiles(0).wait()
    fetch(1).start()
    for t in range(tiles):
        if t == first_tiles:
            fetch_tiles(1).wait()
            fetch_b.wait()
            for i in range(2, len(FETCHES)):
                fetch(i).start()
        same = ids_across[:, t : t + 1] == ids_buf[t : t + 1]
        tile_split[t] = jnp.concatenate(halves(jnp.where(same, tile_buf[t], 0.0)), axis=1)
    gamma = jnp.zeros((nrhs, width), jnp.float32)
    for t in range(tiles):
        value = b_buf[:, cut(t)]
        product = fold(times(split(value), tile_split[t]), nrhs, width)
        u_buf[:, cut(t)] = product
        parts = split(product)
        v_split[:, cut(t)] = parts
        v_minus[:, cut(t)] = -parts
        gamma += value * product
    sums[:nrhs] = gamma
    sums[nrhs:] = jnp.zeros_like(gamma)

    for k, (begin, count) in enumerate(FETCHES):
        fetch(k).wait()
        for q in range(begin, begin + count):
            a_split[q] = split(a_buf[q * width : (q + 1) * width])
            high = times_transposed(v_split[...], a_split[q, :width])
            minus_low = times_transposed(v_minus[...], a_split[q, width:])
            part[0, :, cut(q)] = (high[:nrhs] - minus_low[:nrhs]) + (high[nrhs:] - minus_low[nrhs:])
        if k == 0:
            meet()
        near_group(0, k).start()
        if k >= NEAR_LAG:
            stage1(0, k - NEAR_LAG)
    for k in range(len(FETCHES) - NEAR_LAG, len(FETCHES)):
        stage1(0, k)

    acc[...] = jnp.zeros_like(acc)

    def take(block, q, slot):
        lanes = lanes_of(block, q)
        value = image[0, :, lanes]
        product = fold(times(split(value), tile_split[block * steps + q]), nrhs, width)
        m_buf[:, lanes] = product
        m_split[slot] = split(product)
        sums[nrhs:] += value * u_buf[:, lanes]
        return slot, lanes

    def update(taken, i):
        product = None
        for slot, lanes in taken:
            term = times_transposed(m_split[slot], a_split[i, :, lanes])
            product = term if product is None else product + term
        return acc[:, cut(i)] + fold(product, nrhs, width)

    for q in range(steps):
        stage2(0, q)
    arrivals = [(lane, q) for q in range(steps)] + [(1 - lane, q) for q in range(steps)]
    for q in range(steps):
        carry(0, q)
    taken = []
    for begin in range(0, 2 * steps, 2):
        for k in (begin, begin + 1):
            if k < steps:
                own(0, k)
            else:
                beside(0, k - steps)
        if taken:
            for i in range(steps):
                acc[:, cut(i)] = update(taken, i)
        taken = [take(*arrivals[k], k % 4) for k in (begin, begin + 1)]
    for i in range(steps):
        part[1, :, cut(i)] = update(taken, i)
    for k in range(len(FETCHES)):
        near_group(1, k).start()
    exchange(0, dot_row())
    for k in range(len(FETCHES)):
        stage1(1, k)
    gamma0, delta0 = exchanged(0)
    alpha0 = gamma0 / delta0
    gamma = jnp.zeros((nrhs, width), jnp.float32)
    for t in range(tiles):
        lanes = cut(t)
        res = b_buf[:, lanes] - alpha0 * image[0, :, lanes]
        pre = u_buf[:, lanes] - alpha0 * m_buf[:, lanes]
        gamma += res * pre
    sums[:nrhs] = gamma
    sums[nrhs:] = jnp.zeros_like(gamma)
    exchange(1, dot_row())

    rows = 2 * depth

    def slot_of(origin, target):
        return lax.rem(origin - target + rows, rows)

    def deltas():
        @pl.when(owner)
        def _():
            delta_own[...] = jnp.broadcast_to(dot_row(), delta_own.shape)
            delta_in[0] = delta_own[...]
            for i in range(rows):
                target = lax.rem(my_row + i, rows)
                for shift in range(4):
                    if i or shift:
                        pltpu.make_async_remote_copy(
                            src_ref=delta_own, dst_ref=delta_in.at[slot_of(my_row, target)],
                            send_sem=delta_send.at[0], recv_sem=delta_recv.at[0],
                            device_id=(target, lax.rem(my_col + shift, 4)), device_id_type=MESH,
                        ).start()

    for q in range(steps):
        stage2(1, q)
    for q in range(steps):
        carry(1, q)
        own(1, q)

        @pl.when(owner)
        def _():
            lanes = lanes_of(lane, q)
            img = image[0, :, lanes] - alpha0 * image[1, :, lanes]
            sums[nrhs:] += img * (u_buf[:, lanes] - alpha0 * m_buf[:, lanes])

    deltas()
    for q in range(steps):
        beside(1, q)

    def delta_copy(slots):
        return pltpu.make_async_remote_copy(
            src_ref=slots, dst_ref=slots, send_sem=delta_send.at[0], recv_sem=delta_recv.at[0],
            device_id=(side, my_col), device_id_type=MESH,
        )

    finish(0)
    finish(1)

    @pl.when(owner)
    def _():
        delta_copy(delta_fill).wait_send()
        delta_copy(delta_in.at[pl.ds(1, rows - 1)]).wait_recv()

    @pl.when(others)
    def _():
        delta_copy(delta_in).wait_recv()

    gamma1 = exchanged(1)[0]
    total = delta_in[slot_of(0, my_row)]
    for origin in range(1, rows):
        total = total + delta_in[slot_of(origin, my_row)]
    delta1 = jnp.broadcast_to(total[0:1], (2 * nrhs, width)).T[nrhs:]
    beta = gamma1 / gamma0
    alpha1 = gamma1 / (delta1 - beta * gamma1 / alpha0)
    for t in range(tiles):
        lanes = cut(t)
        u, w = u_buf[:, lanes], image[0, :, lanes]
        pre = u - alpha0 * m_buf[:, lanes]
        img = w - alpha0 * image[1, :, lanes]
        sol_ref[:, lanes] = alpha0 * u + alpha1 * (pre + beta * u)
        res_ref[:, lanes] = (b_buf[:, lanes] - alpha0 * w) - alpha1 * (img + beta * w)


def fused_body(row_count, normal_matrix, right_side, tile_inverse, order_ids):
    block_rows, block_cols = normal_matrix.shape
    nrhs = right_side.shape[1]
    tiles, width = tile_inverse.shape[:2]
    steps = block_rows // width
    depth = row_count // 2
    f32, bf16 = jnp.float32, jnp.bfloat16
    whole = jax.ShapeDtypeStruct((nrhs, block_cols), f32)
    dma = pltpu.SemaphoreType.DMA
    vmem = pl.BlockSpec(memory_space=pltpu.VMEM)
    hbm = pl.BlockSpec(memory_space=pltpu.HBM)
    hh = nrhs // 2
    sol, res = pl.pallas_call(
        functools.partial(kernel, depth, width),
        out_shape=(whole, whole),
        in_specs=[hbm, hbm, hbm, vmem],
        out_specs=(vmem, vmem),
        scratch_shapes=[
            pltpu.VMEM((block_rows, block_cols), f32),
            pltpu.VMEM((steps, 2 * width, block_cols), bf16),
            pltpu.VMEM((tiles, width, width), f32),
            pltpu.VMEM((tiles, width, 2 * width), bf16),
            pltpu.VMEM((2 * nrhs, block_cols), bf16),
            pltpu.VMEM((2 * nrhs, block_cols), bf16),
            pltpu.VMEM((4, 2 * nrhs, width), bf16),
            pltpu.VMEM((nrhs, block_cols), f32),
            pltpu.VMEM((nrhs, block_cols), f32),
            pltpu.VMEM((nrhs, block_cols), f32),
            pltpu.VMEM((2, nrhs, block_rows), f32),
            pltpu.VMEM((2, hh, block_rows), f32),
            pltpu.VMEM((2, hh, block_rows), f32),
            pltpu.VMEM((2, hh, block_rows), f32),
            pltpu.VMEM((2, hh, block_rows), f32),
            pltpu.VMEM((2, hh, block_rows), f32),
            pltpu.VMEM((2, nrhs, block_cols), f32),
            pltpu.VMEM((nrhs, block_rows), f32),
            pltpu.VMEM((2 * nrhs, width), f32),
            pltpu.VMEM((2, 8, width), f32),
            pltpu.VMEM((2, 3, 8, width), f32),
            pltpu.VMEM((8, width), f32),
            pltpu.VMEM((8 * depth - 1, 8, width), f32),
            pltpu.VMEM((2 * depth, 8, width), f32),
            pltpu.VMEM((width, width), f32),
            dma((len(FETCHES),)),
            dma((3,)),
            dma((2, len(FETCHES))),
            dma((2, steps)),
            dma((2, steps)),
            dma((2, steps)),
            dma((2, steps)),
            dma((2,)),
            dma((2,)),
            dma((2,)),
            dma((2,)),
            dma((2, 4)),
            dma((2, 2)),
            dma((2,)),
            dma((2,)),
            dma((1,)),
            dma((1,)),
        ],
        compiler_params=pltpu.CompilerParams(
            collective_id=0, has_side_effects=True, vmem_limit_bytes=53500 * 1024
        ),
    )(normal_matrix, tile_inverse, right_side.T, order_ids.reshape(tiles, width))
    return sol.T, res.T


def body(row_count, col_count, normal_matrix, right_side, tile_inverse, order_ids):
    block_rows, block_cols = normal_matrix.shape
    width = tile_inverse.shape[1]
    fits = (
        col_count == 4
        and row_count == 8
        and block_cols == 2 * block_rows
        and block_rows % width == 0
        and width == 128
        and block_rows == width * (FETCHES[-1][0] + FETCHES[-1][1])
        and tile_inverse.shape[0] <= width
        and right_side.shape[1] == 64
    )
    if fits:
        return fused_body(row_count, normal_matrix, right_side, tile_inverse, order_ids)
    return plain_body(normal_matrix, right_side, tile_inverse, order_ids)


def solution(mesh):
    return jax.shard_map(
        functools.partial(body, mesh.shape["row"], mesh.shape["col"]),
        mesh=mesh,
        in_specs=(P("row", "col"), P("col", None), P("col", None, None), P("col")),
        out_specs=(P("col", None), P("col", None)),
        check_vma=False,
    )
```
